32 devices in a mesh: dp: 2 (over z, core), sp: 16 (over x, y).
Axes of the slice: x: 4, y: 4, z: 1, core: 2. Of those that a mesh axis runs over, the one named last changes fastest.
The devices are a block of a 4x4x8 slice.
Arguments:
- x: bfloat16 [8192, 5376], P(('dp', 'sp')), parts along dimension 0
- gain: bfloat16 [5376], replicated
- wq: bfloat16 [5376, 4096], replicated
- wk: bfloat16 [5376, 2048], replicated
- wv: bfloat16 [5376, 2048], replicated
- wo: bfloat16 [4096, 5376], replicated
Outputs:
- output: bfloat16 [8192, 5376], P(('dp', 'sp')), parts along dimension 0
There are 2 independent parts. The reference program is written for one: setup_inputs(seed, part) draws one part's arguments, and reference() takes and returns one part's arrays. A program takes and returns all parts, laid end to end along the dimension named above; an argument that names none is the same for every part.
All inputs are finite; a program needn't handle non-finite values.
Results may differ from the reference program's by a relative error of at most 0.012.
Values are sent between devices in bfloat16 or wider.
A program may use at most 768 MiB of HBM per device.

```python
import jax
import jax.numpy as jnp
from jax import lax

ROWS = 4096
D = 5376
HEADS = 32
KV_HEADS = 16
HEAD = 128
THETA = 10000


def setup_inputs(seed: int = 0, part: int = 0) -> dict:
    kx, kn, kq, kk, kv, ko = jax.random.split(jax.random.key(seed), 6)

    def weights(key, rows, columns):
        return jax.random.normal(key, (rows, columns), jnp.float32) * rows**-0.5

    drawn = {
        "x": jax.random.normal(jax.random.fold_in(kx, part), (ROWS, D), jnp.float32),
        "gain": 1 + 0.1 * jax.random.normal(kn, (D,), jnp.float32),
        "wq": 2 * weights(kq, D, HEADS * HEAD),
        "wk": 2 * weights(kk, D, KV_HEADS * HEAD),
        "wv": 4 * weights(kv, D, KV_HEADS * HEAD),
        "wo": weights(ko, HEADS * HEAD, D),
    }
    return {k: v.astype(jnp.bfloat16) for k, v in drawn.items()}


def normed(x, gain):
    wide = x.astype(jnp.float32)
    scale = lax.rsqrt(jnp.mean(wide * wide, -1, keepdims=True) + 1e-6)
    return (wide * scale * gain.astype(jnp.float32)).astype(jnp.bfloat16)


def turned(t, place, theta):
    half = t.shape[-1] // 2
    angle = place.astype(jnp.float32)[:, None] * theta ** (-jnp.arange(half, dtype=jnp.float32) / half)
    cos, sin = jnp.cos(angle)[:, None], jnp.sin(angle)[:, None]
    a, b = t[..., :half].astype(jnp.float32), t[..., half:].astype(jnp.float32)
    return jnp.concatenate([a * cos - b * sin, b * cos + a * sin], -1).astype(jnp.bfloat16)


def matmul(a, w):
    return jnp.dot(a, w, preferred_element_type=jnp.float32).astype(jnp.bfloat16)


def einsum(form, a, b):
    return jnp.einsum(form, a.astype(jnp.float32), b.astype(jnp.float32))


def attention(q, k, v):
    scores = einsum("tgsd,ugd->gstu", q, k) * q.shape[-1] ** -0.5
    token = jnp.arange(q.shape[0])
    scores = jnp.where(token[:, None] >= token, scores, -jnp.inf)
    weights = jax.nn.softmax(scores, -1).astype(jnp.bfloat16)
    return einsum("gstu,ugd->tgsd", weights, v).astype(jnp.bfloat16)


def reference(x, gain, wq, wk, wv, wo):
    a, place = normed(x, gain), jnp.arange(ROWS)
    q = turned(matmul(a, wq).reshape(ROWS, HEADS, HEAD), place, THETA).reshape(ROWS, KV_HEADS, -1, HEAD)
    k = turned(matmul(a, wk).reshape(ROWS, KV_HEADS, HEAD), place, THETA)
    v = matmul(a, wv).reshape(ROWS, KV_HEADS, HEAD)
    seen = attention(q, k, v).reshape(ROWS, HEADS * HEAD)
    return (x.astype(jnp.float32) + jnp.dot(seen, wo, preferred_element_type=jnp.float32)).astype(jnp.bfloat16)
```

```python
import functools
import math

import jax
import jax.numpy as jnp
from jax import lax
from jax.experimental import pallas as pl
from jax.experimental.pallas import tpu as pltpu
from jax.sharding import PartitionSpec as P

HEAD = 128
THETA = 10000
NEG = -1e30
HIDDEN = 2 * NEG
LOG2E = 1.4426950408889634
VMEM = 67043328
SLOTS = 12
AHEAD = 4
MESH = pl.DeviceIdType.MESH

STEPS = [(1, 1), (3, 3), (0, 1), (0, 3), (1, 3), (3, 1), (1, 0), (3, 0), (1, 2), (3, 2), (2, 1), (2, 3), (2, 2), (2, 0), (0, 2), (0, 0)]


def _packed(values):
    return [sum(v << (2 * i) for i, v in enumerate(values[at : at + 8])) for at in (0, 8)]


def _look(table, s):
    low, high = table
    word = jnp.where(s < 8, jnp.int32(low), jnp.int32(high))
    return lax.shift_right_logical(word, 2 * lax.rem(s, 8)) & 3


def _dot(a, b):
    return jnp.dot(a, b, preferred_element_type=jnp.float32)


def _kernel(n, x_ref, gain_ref, cos_ref, sin_ref, wq, wk, wv, wo, y_ref,
            a_s, w_s, k_out, v_out, q_out, k_in, v_in, q_in, o_out, o_in, s_s, mix_s, gap_s,
            w_sem, k_sent, k_got, v_sent, v_got, q_sent, q_got, o_sent, o_got):
    own, depth = x_ref.shape
    features = wo.shape[0]
    hk, hq = k_out.shape[2], o_out.shape[2]
    g = hq // hk
    cols = g * own
    bk = s_s.shape[1]
    per = bk // own
    blocks = depth // hq
    side = math.isqrt(n)
    me = lax.axis_index("sp")
    mx, my = lax.div(me, side), lax.rem(me, side)
    xs, ys = _packed([s[0] for s in STEPS]), _packed([s[1] for s in STEPS])
    e = hk**-0.5 * LOG2E

    def target(s):
        return lax.rem(mx + _look(xs, s), side) * side + lax.rem(my + _look(ys, s), side)

    def source(s):
        return lax.rem(mx - _look(xs, s) + side, side) * side + lax.rem(my - _look(ys, s) + side, side)

    barrier = pltpu.get_barrier_semaphore()
    for s in range(1, n):
        pl.semaphore_signal(barrier, inc=1, device_id={"sp": lax.rem(me + s, n)}, device_id_type=MESH)

    def fetch_kv(t):
        slot, at = lax.rem(t, SLOTS), pl.ds(pl.multiple_of(target(t) * hk, hk), hk)
        pltpu.make_async_copy(wk.at[:, at], w_s.at[slot, pl.ds(0, depth), pl.ds(0, hk)], w_sem.at[slot]).start()
        pltpu.make_async_copy(wv.at[:, at], w_s.at[slot, pl.ds(0, depth), pl.ds(hk, hk)], w_sem.at[slot]).start()

    def q_copy(t):
        slot, at = lax.rem(t, SLOTS), pl.ds(pl.multiple_of(target(t - n) * hq, hq), hq)
        return pltpu.make_async_copy(wq.at[:, at], w_s.at[slot, pl.ds(0, depth), :], w_sem.at[slot])

    def o_copy(b):
        slot, at = lax.rem(b + 2 * n, SLOTS), pl.ds(pl.multiple_of(b * hq, hq), hq)
        return pltpu.make_async_copy(wo.at[:, at], w_s.at[slot, pl.ds(0, features), :], w_sem.at[slot])

    lax.fori_loop(0, AHEAD, lambda t, _: fetch_kv(t), None)

    rows = 16

    def norm(r, _):
        at = pl.ds(pl.multiple_of(r * rows, rows), rows)
        wide = x_ref[at, :].astype(jnp.float32)
        scale = lax.rsqrt(jnp.mean(wide * wide, -1, keepdims=True) + 1e-6)
        a_s[at, :] = (wide * scale * gain_ref[...]).astype(a_s.dtype)

    lax.fori_loop(0, own // rows, norm, None)
    gap_s[...] = lax.rem(lax.broadcasted_iota(jnp.int32, (bk, cols), 1), own) - lax.broadcasted_iota(jnp.int32, (bk, cols), 0)
    v_in[:, hk:, :] = jnp.ones((n, v_in.shape[1] - hk, own), v_in.dtype)
    pl.semaphore_wait(barrier, n - 1)

    def turned(t):
        wide = t.astype(jnp.float32)
        return (wide * cos_ref[...] + pltpu.roll(wide, hk // 2, 1) * sin_ref[...]).astype(t.dtype)

    def send(src, dst, sent, got, to, frm):
        return pltpu.make_async_remote_copy(src_ref=src, dst_ref=dst, send_sem=sent.at[to], recv_sem=got.at[frm],
                                            device_id={"sp": to}, device_id_type=MESH)

    def k_send(to, frm):
        return send(k_out.at[to], k_in.at[frm], k_sent, k_got, to, frm)

    def v_send(to, frm):
        return send(v_out.at[to], v_in.at[frm, pl.ds(0, hk), :], v_sent, v_got, to, frm)

    def q_send(to, frm):
        return send(q_out.at[to], q_in.at[frm], q_sent, q_got, to, frm)

    def o_send(to, frm):
        return send(o_out.at[to], o_in.at[:, pl.ds(pl.multiple_of(frm * hq, hq), hq)], o_sent, o_got, to, frm)

    def keys_values(t, _):
        slot, to = lax.rem(t, SLOTS), target(t)

        @pl.when(t + AHEAD < n)
        def _():
            fetch_kv(t + AHEAD)

        @pl.when(t + AHEAD >= n)
        def _():
            q_copy(t + AHEAD).start()

        pltpu.make_async_copy(
            wq.at[:, pl.ds(0, hq)], w_s.at[slot, pl.ds(0, depth), :], w_sem.at[slot]).wait()
        r = _dot(a_s[...], w_s[slot, :depth, :]).astype(a_s.dtype)

        @pl.when(t > 0)
        def _():
            before = target(jnp.maximum(t - 1, 0))
            k_send(before, me).start()
            v_send(before, me).start()

        k, v = turned(r[:, :hk]), r[:, hk:].T

        @pl.when(t < n - 1)
        def _():
            k_out[to] = k
            v_out[to] = v

        @pl.when(t == n - 1)
        def _():
            k_in[me] = k
            v_in[me, :hk, :] = v

    lax.fori_loop(0, n, keys_values, None)

    def queries(t, _):
        s = t - n
        slot, to = lax.rem(t, SLOTS), target(s)

        @pl.when(t + AHEAD < 2 * n)
        def _():
            q_copy(t + AHEAD).start()

        @pl.when(t + AHEAD >= 2 * n)
        def _():
            o_copy(t + AHEAD - 2 * n).start()

        q_copy(t).wait()
        r = _dot(a_s[...], w_s[slot, :depth, :]).astype(a_s.dtype)

        @pl.when(s > 0)
        def _():
            q_send(target(jnp.maximum(s - 1, 0)), me).start()

        q = [turned(r[:, h * hk : (h + 1) * hk]).T for h in range(g)]

        @pl.when(s < n - 1)
        def _():
            for h in range(g):
                q_out[to, :, h * own : (h + 1) * own] = q[h]

        @pl.when(s == n - 1)
        def _():
            for h in range(g):
                q_in[me, :, h * own : (h + 1) * own] = q[h]

    lax.fori_loop(n, 2 * n, queries, None)

    def got_keys(s, _):
        frm = source(s)
        k_send(frm, frm).wait_recv()
        v_send(frm, frm).wait_recv()

    lax.fori_loop(0, n - 1, got_keys, None)

    def attend(s, _):
        i = source(lax.rem(s + n - 1, n))

        @pl.when(s > 0)
        def _():
            q_send(i, i).wait_recv()

        @pl.when(AHEAD + s < SLOTS)
        def _():
            o_copy(AHEAD + s).start()

        def scores(j):
            keys = jnp.concatenate([k_in[j * per + c] for c in range(per)], axis=0)
            s_s[lax.rem(j, 2)] = _dot(keys, q_in[i])

        def take(j, top, masked):
            sc = s_s[lax.rem(j, 2)]
            if masked:
                sc = jnp.where(gap_s[...] >= j * bk - i * own, sc, HIDDEN)
            new = jnp.maximum(top, sc.max(axis=0, keepdims=True))
            p = jnp.exp2((sc - new) * e).astype(k_in.dtype)
            keep = jnp.exp2((top - new) * e)
            values = jnp.concatenate([v_in[j * per + c] for c in range(per)], axis=1)
            mix_s[...] = mix_s[...] * keep + _dot(values, p)
            return new

        scores(0)

        @pl.when(s > 1)
        def _():
            o_send(source(jnp.maximum(s - 2, 0)), me).start()

        mix_s[...] = jnp.zeros_like(mix_s)
        last = lax.div(i, per)

        def block(j, top):
            scores(j + 1)
            return take(j, top, False)

        top = lax.fori_loop(0, last, block, jnp.full((1, cols), NEG, jnp.float32))
        take(last, top, True)
        out = (mix_s[:hk, :] * (1 / mix_s[hk : hk + 1, :])).astype(o_in.dtype)
        out = jnp.concatenate([out[:, h * own : (h + 1) * own].T for h in range(g)], axis=1)

        @pl.when(s > 0)
        def _():
            o_out[i] = out

        @pl.when(s == 0)
        def _():
            o_in[:, pl.ds(pl.multiple_of(me * hq, hq), hq)] = out

    lax.fori_loop(0, n, attend, None)
    o_send(source(n - 2), me).start()

    def got_rest(s, _):
        frm = target(s)
        o_send(frm, frm).wait_recv()

    lax.fori_loop(0, n - 1, got_rest, None)

    def project(b, _):
        o_copy(b).wait()
        at = pl.ds(pl.multiple_of(b * hq, hq), hq)
        r = _dot(o_in[...], w_s[lax.rem(b + 2 * n, SLOTS), :features, :])
        y_ref[:, at] = (x_ref[:, at].astype(jnp.float32) + r).astype(y_ref.dtype)

        @pl.when(b + SLOTS < blocks)
        def _():
            o_copy(b + SLOTS).start()

    lax.fori_loop(0, blocks, project, None)

    def gone(s, _):
        to = target(s)
        k_send(to, me).wait_send()
        v_send(to, me).wait_send()
        q_send(to, me).wait_send()
        o_send(to, me).wait_send()

    lax.fori_loop(0, n - 1, gone, None)


def solution(mesh):
    n = mesh.shape["sp"]

    def step(x, gain, wq, wk, wv, wo):
        own, depth = x.shape
        hq, hk, features = wq.shape[1] // n, wk.shape[1] // n, wo.shape[0]
        g = hq // hk
        low = x.dtype
        half = HEAD // 2
        place = (lax.axis_index("sp") * own + jnp.arange(own)).astype(jnp.float32)
        angle = place[:, None] * THETA ** (-jnp.arange(half, dtype=jnp.float32) / half)
        cos, sin = jnp.cos(angle), jnp.sin(angle)
        cos, sin = jnp.concatenate([cos, cos], -1), jnp.concatenate([-sin, sin], -1)
        bk = 2 * own
        sems = pltpu.SemaphoreType.DMA((n,))
        vmem, hbm = pl.BlockSpec(memory_space=pltpu.VMEM), pl.BlockSpec(memory_space=pl.ANY)
        return pl.pallas_call(
            functools.partial(_kernel, n),
            name="half_layer",
            out_shape=jax.ShapeDtypeStruct((own, depth), low),
            in_specs=[vmem] * 4 + [hbm] * 4,
            out_specs=vmem,
            scratch_shapes=[
                pltpu.VMEM((own, depth), low),
                pltpu.VMEM((SLOTS, max(depth, features), hq), low),
                pltpu.VMEM((n, own, hk), low),
                pltpu.VMEM((n, hk, own), low),
                pltpu.VMEM((n, hk, g * own), low),
                pltpu.VMEM((n, own, hk), low),
                pltpu.VMEM((n, hk + 16, own), low),
                pltpu.VMEM((n, hk, g * own), low),
                pltpu.VMEM((n, own, hq), low),
                pltpu.VMEM((own, n * hq), low),
                pltpu.VMEM((2, bk, g * own), jnp.float32),
                pltpu.VMEM((hk + 16, g * own), jnp.float32),
                pltpu.VMEM((bk, g * own), jnp.int32),
                pltpu.SemaphoreType.DMA((SLOTS,)),
            ] + [sems] * 8,
            compiler_params=pltpu.CompilerParams(collective_id=0, has_side_effects=True, vmem_limit_bytes=VMEM),
        )(x, gain.astype(jnp.float32)[None], cos, sin, wq, wk, wv, wo)

    tokens, whole = P(("dp", "sp"), None), P(None, None)
    return jax.shard_map(
        step,
        mesh=mesh,
        in_specs=(tokens, P(None), whole, whole, whole, whole),
        out_specs=tokens,
        check_vma=False,
    )
```

```python
import functools
import math

import jax
import jax.numpy as jnp
from jax import lax
from jax.experimental import pallas as pl
from jax.experimental.pallas import tpu as pltpu
from jax.sharding import PartitionSpec as P

HEAD = 128
THETA = 10000
NEG = -1e30
HIDDEN = 2 * NEG
LOG2E = 1.4426950408889634
VMEM = 67043328
SLOTS = 11
JOIN = 3
AHEAD = 6
MESH = pl.DeviceIdType.MESH

STEPS = [(1, 1), (3, 3), (1, 3), (3, 1), (1, 0), (3, 0), (0, 1), (0, 3), (1, 2), (3, 2), (2, 1), (2, 3), (2, 2), (2, 0), (0, 2), (0, 0)]
UNITS = [(3, 0), (1, 0), (3, 1), (1, 1), (2, 1), (2, 0), (0, 1), (0, 0)]
NEAR = [3, 0, 2, 1]


def _packed(values):
    return sum(v << (2 * i) for i, v in enumerate(values))


def _look(word, i):
    return lax.shift_right_logical(jnp.int32(word), 2 * i) & 3


def _step(axis, t):
    low, high = (_packed([s[axis] for s in STEPS[at : at + 8]]) for at in (0, 8))
    return lax.shift_right_logical(jnp.where(t < 8, jnp.int32(low), jnp.int32(high)), 2 * lax.rem(t, 8)) & 3


def _dot(a, b):
    return jnp.dot(a, b, preferred_element_type=jnp.float32)


def _kernel(n, x_ref, gain_ref, cos_ref, sin_ref, wq, wk, wv, wo, y_ref,
            a_s, w_s, k_out, v_out, q_out, k_in, v_in, q_in, o_out, o_in, even_s, odd_s, mix_s, top_s, sum_s,
            w_sem, y_sem, k_sent, k_got, v_sent, v_got, q_sent, q_got, o_sent, o_got):
    own, depth = x_ref.shape
    features = wo.shape[0]
    hk, hq = k_out.shape[2], o_out.shape[2]
    g = hq // hk
    cols = g * own
    bk = even_s.shape[0]
    per = bk // own
    blocks = depth // hq
    me = lax.axis_index("sp")
    e = hk**-0.5 * LOG2E

    side = math.isqrt(n)
    mx, my = lax.div(me, side), lax.rem(me, side)
    row = features // side

    def target(t):
        return lax.rem(mx + _step(0, t), side) * side + lax.rem(my + _step(1, t), side)

    def unit(i):
        flip = _look(_packed([s[1] for s in UNITS]), i)
        return lax.div(lax.rem(mx + _look(_packed([s[0] for s in UNITS]), i), side) * side, per) + (lax.div(my, per) ^ flip)

    def place(to, frm):
        rows = lax.rem(lax.div(frm, side) - lax.div(to, side) + side, side)
        return _look(_packed(NEAR), rows) * side + lax.rem(frm, side)

    barrier = pltpu.get_barrier_semaphore()
    for s in range(1, n):
        pl.semaphore_signal(barrier, inc=1, device_id={"sp": lax.rem(me + s, n)}, device_id_type=MESH)

    def fetch_kv(t):
        slot, at = lax.rem(t, SLOTS), pl.ds(pl.multiple_of(target(t) * hk, hk), hk)
        pltpu.make_async_copy(wk.at[:, at], w_s.at[slot, pl.ds(0, depth), pl.ds(0, hk)], w_sem.at[slot]).start()
        pltpu.make_async_copy(wv.at[:, at], w_s.at[slot, pl.ds(0, depth), pl.ds(hk, hk)], w_sem.at[slot]).start()

    def q_copy(t):
        slot, at = lax.rem(t, SLOTS), pl.ds(pl.multiple_of(target(t - n) * hq, hq), hq)
        return pltpu.make_async_copy(wq.at[:, at], w_s.at[slot, pl.ds(0, depth), :], w_sem.at[slot])

    near = (blocks + 1) // 2
    jobs = near + 2 * (blocks // JOIN)

    def o_slot(j):
        return lax.rem(j + 2 * n, SLOTS)

    def fetch_o(j):
        slot = o_slot(j)

        @pl.when(j < near)
        def _():
            for b in range(2):
                @pl.when(2 * j + b < blocks)
                def _():
                    at = pl.ds(pl.multiple_of((2 * j + b) * hq, hq), hq)
                    for step in (1, side - 1):
                        frm = pl.multiple_of(lax.rem(mx + step, side) * row, row)
                        into = pl.ds((2 * b + NEAR[step]) * row, row)
                        pltpu.make_async_copy(wo.at[pl.ds(frm, row), at], w_s.at[slot, into, :], w_sem.at[slot]).start()

        @pl.when(j >= near)
        def _():
            far = j < near + blocks // JOIN
            frm = pl.multiple_of(jnp.where(far, lax.rem(mx + 2, side), mx) * row, row)
            first = jnp.where(far, j - near, j - near - blocks // JOIN) * JOIN
            for b in range(JOIN):
                at = pl.ds(pl.multiple_of((first + b) * hq, hq), hq)
                pltpu.make_async_copy(wo.at[pl.ds(frm, row), at], w_s.at[slot, pl.ds(b * row, row), :], w_sem.at[slot]).start()

    def o_here(j, rows):
        slot, rows = o_slot(j), pl.ds(0, rows)
        pltpu.make_async_copy(wo.at[rows, pl.ds(0, hq)], w_s.at[slot, rows, :], w_sem.at[slot]).wait()
        return slot

    lax.fori_loop(0, AHEAD, lambda t, _: fetch_kv(t), None)

    rows = 16

    def norm(r, _):
        at = pl.ds(pl.multiple_of(r * rows, rows), rows)
        wide = x_ref[at, :].astype(jnp.float32)
        scale = lax.rsqrt(jnp.mean(wide * wide, -1, keepdims=True) + 1e-6)
        a_s[at, :] = (wide * scale * gain_ref[...].astype(jnp.float32)[None]).astype(a_s.dtype)

    lax.fori_loop(0, own // rows, norm, None, unroll=4)
    v_in[:, hk:, :] = jnp.ones((n, v_in.shape[1] - hk, own), v_in.dtype)
    pl.semaphore_wait(barrier, n - 1)

    def turned(t):
        wide = t.astype(jnp.float32)
        return (wide * cos_ref[...] + pltpu.roll(wide, hk // 2, 1) * sin_ref[...]).astype(t.dtype)

    def send(src, dst, sent, got, to, frm):
        return pltpu.make_async_remote_copy(src_ref=src, dst_ref=dst, send_sem=sent.at[to], recv_sem=got.at[frm],
                                            device_id={"sp": to}, device_id_type=MESH)

    def k_send(to, frm):
        return send(k_out.at[to], k_in.at[frm], k_sent, k_got, to, frm)

    def v_send(to, frm):
        return send(v_out.at[to], v_in.at[frm, pl.ds(0, hk), :], v_sent, v_got, to, frm)

    def q_send(to, frm):
        return send(q_out.at[to], q_in.at[frm], q_sent, q_got, to, frm)

    def o_send(to, frm):
        return send(o_out.at[to], o_in.at[place(to, frm)], o_sent, o_got, to, frm)

    def block_here(t):
        slot = lax.rem(t, SLOTS)
        pltpu.make_async_copy(wq.at[:, pl.ds(0, hq)], w_s.at[slot, pl.ds(0, depth), :], w_sem.at[slot]).wait()
        return slot

    def made(t):
        return _dot(a_s[...], w_s[lax.rem(t, SLOTS), :depth, :]).astype(a_s.dtype)

    def keys_values(i, _):
        for t in (2 * i, 2 * i + 1):
            @pl.when(t + AHEAD < n)
            def _():
                fetch_kv(t + AHEAD)

            @pl.when(t + AHEAD >= n)
            def _():
                q_copy(t + AHEAD).start()

        @pl.when(i > 0)
        def _():
            before = target(jnp.maximum(2 * i - 1, 0))
            k_send(before, me).start()
            v_send(before, me).start()

        for t in (2 * i, 2 * i + 1):
            block_here(t)

        def finish(to, r):
            k_out[to] = turned(r[:, :hk])
            v_out[to] = r[:, hk:].T

        first, second = target(2 * i), target(2 * i + 1)
        finish(first, made(2 * i))
        r = made(2 * i + 1)
        k_send(first, me).start()
        v_send(first, me).start()
        finish(second, r)

    lax.fori_loop(0, n // 2, keys_values, None)
    k_in[me] = k_out[me]
    v_in[me, :hk, :] = v_out[me]

    def queries(i, _):
        for t in (2 * i, 2 * i + 1):
            @pl.when(t + n + AHEAD < 2 * n)
            def _():
                q_copy(t + n + AHEAD).start()

            @pl.when(t + n + AHEAD >= 2 * n)
            def _():
                fetch_o(t + AHEAD - n)

        @pl.when(i > 0)
        def _():
            q_send(target(jnp.maximum(2 * i - 1, 0)), me).start()

        for t in (2 * i, 2 * i + 1):
            block_here(t + n)

        def finish(to, r):
            for h in range(g):
                q_out[to, :, h * own : (h + 1) * own] = turned(r[:, h * hk : (h + 1) * hk]).T

        first, second = target(2 * i), target(2 * i + 1)
        finish(first, made(2 * i + n))
        r = made(2 * i + 1 + n)
        q_send(first, me).start()
        finish(second, r)

    lax.fori_loop(0, n // 2, queries, None)
    q_in[me] = q_out[me]

    def got_keys(s, _):
        frm = target(s)
        k_send(frm, frm).wait_recv()
        v_send(frm, frm).wait_recv()

    lax.fori_loop(0, n - 1, got_keys, None)

    def attend(s, _):
        u = unit(s)

        @pl.when(AHEAD + s < SLOTS)
        def _():
            fetch_o(AHEAD + s)

        @pl.when(s > 0)
        def _():
            send_out(jnp.maximum(s - 1, 0))

        for c in range(per):
            @pl.when(per * u + c != me)
            def _():
                q_send(per * u + c, per * u + c).wait_recv()

        def scores(j, into):
            keys = jnp.concatenate([k_in[j * per + c] for c in range(per)], axis=0)
            for c in range(per):
                into[:, c * cols : (c + 1) * cols] = _dot(keys, q_in[u * per + c])

        def take(j, held, masked):
            weights, keeps = [], []
            for c in range(per):
                at = slice(c * cols, (c + 1) * cols)
                sc = held[:, at]
                if masked:
                    query = lax.rem(lax.broadcasted_iota(jnp.int32, (bk, cols), 1), own) + c * own
                    sc = jnp.where(query >= lax.broadcasted_iota(jnp.int32, (bk, cols), 0), sc, HIDDEN)
                old = top_s[:, at]
                new = jnp.maximum(old, sc.max(axis=0, keepdims=True))
                top_s[:, at] = new
                weights.append(jnp.exp2((sc - new) * e).astype(k_in.dtype))
                keeps.append(jnp.exp2((old - new) * e))
            values = jnp.concatenate([v_in[j * per + c] for c in range(per)], axis=1)
            for c in range(per):
                at = slice(c * cols, (c + 1) * cols)
                mix_s[:, at] = mix_s[:, at] * keeps[c] + _dot(values, weights[c])

        scores(0, even_s)

        mix_s[...] = jnp.zeros_like(mix_s)
        top_s[...] = jnp.full_like(top_s, NEG)

        def two(i, _):
            scores(2 * i + 1, odd_s)
            take(2 * i, even_s, False)
            scores(2 * i + 2, even_s)
            take(2 * i + 1, odd_s, False)

        lax.fori_loop(0, lax.div(u, 2), two, None)

        @pl.when(lax.rem(u, 2) == 1)
        def _():
            scores(u, odd_s)
            take(u - 1, even_s, False)
            take(u, odd_s, True)

        @pl.when(lax.rem(u, 2) == 0)
        def _():
            take(u, even_s, True)

        for c in range(per):
            at = slice(c * cols, (c + 1) * cols)
            out = (mix_s[:hk, at] * (1 / mix_s[hk : hk + 1, at])).astype(o_in.dtype)
            o_out[per * u + c] = jnp.concatenate([out[:, h * own : (h + 1) * own].T for h in range(g)], axis=1)

    def send_out(s):
        u = unit(s)
        for c in range(per):
            @pl.when(per * u + c != me)
            def _():
                o_send(per * u + c, me).start()

    lax.fori_loop(0, n // 2, attend, None)
    send_out(n // 2 - 1)
    o_in[place(me, me)] = o_out[me]

    def got_out(first, last):
        def got(t, _):
            frm = target(t)

            @pl.when((_stands(frm) >= first) & (_stands(frm) < last))
            def _():
                pltpu.make_async_remote_copy(src_ref=o_out.at[frm], dst_ref=o_in.at[place(me, frm)], send_sem=o_sent.at[frm],
                                             recv_sem=o_got.at[frm], device_id={"sp": frm}, device_id_type=MESH).wait_recv()

        lax.fori_loop(0, n - 1, got, None)

    def _stands(frm):
        return lax.div(place(me, frm), side)

    def results(first, last):
        return jnp.concatenate([o_in[i] for i in range(first * side, last * side)], axis=1)

    got_out(0, 2)

    def rows_near(i, count):
        slot = o_here(i, 2 * row * count)
        for b in range(count):
            at = pl.ds(pl.multiple_of((2 * i + b) * hq, hq), hq)
            r = _dot(results(0, 2), w_s[slot, 2 * b * row : 2 * (b + 1) * row, :])
            sum_s[:, at] = x_ref[:, at].astype(jnp.float32) + r

        @pl.when(i + SLOTS < jobs)
        def _():
            fetch_o(i + SLOTS)

    lax.fori_loop(0, blocks // 2, lambda i, _: rows_near(i, 2), None)
    if blocks % 2:
        rows_near(blocks // 2, 1)
    got_out(2, 3)

    def row_far(i, _):
        slot = o_here(near + i, JOIN * row)
        for b in range(JOIN):
            at = pl.ds(pl.multiple_of((i * JOIN + b) * hq, hq), hq)
            sum_s[:, at] += _dot(results(2, 3), w_s[slot, b * row : (b + 1) * row, :])

        @pl.when(near + i + SLOTS < jobs)
        def _():
            fetch_o(near + i + SLOTS)

    lax.fori_loop(0, blocks // JOIN, row_far, None)
    got_out(3, 4)

    def y_copy(i):
        at = pl.ds(pl.multiple_of(i * JOIN * hq, JOIN * hq), JOIN * hq)
        return pltpu.make_async_copy(a_s.at[:, at], y_ref.at[:, at], y_sem.at[i])

    def project(i, _):
        slot = o_here(near + blocks // JOIN + i, JOIN * row)

        for b in range(JOIN):
            at = pl.ds(pl.multiple_of((i * JOIN + b) * hq, hq), hq)
            r = _dot(results(3, 4), w_s[slot, b * row : (b + 1) * row, :])
            a_s[:, at] = (sum_s[:, at] + r).astype(a_s.dtype)

        @pl.when(i > 0)
        def _():
            y_copy(jnp.maximum(i - 1, 0)).start()

    lax.fori_loop(0, blocks // JOIN, project, None)
    y_copy(blocks // JOIN - 1).start()

    def gone(s, _):
        to = target(s)
        k_send(to, me).wait_send()
        v_send(to, me).wait_send()
        q_send(to, me).wait_send()
        o_send(to, me).wait_send()

    lax.fori_loop(0, n - 1, gone, None)
    lax.fori_loop(0, blocks // JOIN, lambda i, _: y_copy(i).wait(), None)


def solution(mesh):
    n = mesh.shape["sp"]

    def step(x, gain, wq, wk, wv, wo):
        own, depth = x.shape
        hq, hk, features = wq.shape[1] // n, wk.shape[1] // n, wo.shape[0]
        g = hq // hk
        low = x.dtype
        half = HEAD // 2
        place = (lax.axis_index("sp") * own + jnp.arange(own)).astype(jnp.float32)
        angle = place[:, None] * THETA ** (-jnp.arange(half, dtype=jnp.float32) / half)
        cos, sin = jnp.cos(angle), jnp.sin(angle)
        cos, sin = jnp.concatenate([cos, cos], -1), jnp.concatenate([-sin, sin], -1)
        bk = 2 * own
        sems = pltpu.SemaphoreType.DMA((n,))
        vmem, hbm = pl.BlockSpec(memory_space=pltpu.VMEM), pl.BlockSpec(memory_space=pl.ANY)
        return pl.pallas_call(
            functools.partial(_kernel, n),
            name="half_layer",
            out_shape=jax.ShapeDtypeStruct((own, depth), low),
            in_specs=[vmem] * 4 + [hbm] * 4,
            out_specs=hbm,
            scratch_shapes=[
                pltpu.VMEM((own, depth), low),
                pltpu.VMEM((SLOTS, max(depth, features), hq), low),
                pltpu.VMEM((n, own, hk), low),
                pltpu.VMEM((n, hk, own), low),
                pltpu.VMEM((n, hk, g * own), low),
                pltpu.VMEM((n, own, hk), low),
                pltpu.VMEM((n, hk + 16, own), low),
                pltpu.VMEM((n, hk, g * own), low),
                pltpu.VMEM((n, own, hq), low),
                pltpu.VMEM((n, own, hq), low),
                pltpu.VMEM((bk, 2 * g * own), jnp.float32),
                pltpu.VMEM((bk, 2 * g * own), jnp.float32),
                pltpu.VMEM((hk + 16, 2 * g * own), jnp.float32),
                pltpu.VMEM((1, 2 * g * own), jnp.float32),
                pltpu.VMEM((own, depth), jnp.float32),
                pltpu.SemaphoreType.DMA((SLOTS,)),
                pltpu.SemaphoreType.DMA((depth // hq // JOIN,)),
            ] + [sems] * 8,
            compiler_params=pltpu.CompilerParams(collective_id=0, has_side_effects=True, vmem_limit_bytes=VMEM),
        )(x, gain, cos, sin, wq, wk, wv, wo)

    tokens, whole = P(("dp", "sp"), None), P(None, None)
    return jax.shard_map(
        step,
        mesh=mesh,
        in_specs=(tokens, P(None), whole, whole, whole, whole),
        out_specs=tokens,
        check_vma=False,
    )
```

```python
import functools
import math

import jax
import jax.numpy as jnp
from jax import lax
from jax.experimental import pallas as pl
from jax.experimental.pallas import tpu as pltpu
from jax.sharding import PartitionSpec as P

HEAD = 128
THETA = 10000
NEG = -1e30
HIDDEN = 2 * NEG
LOG2E = 1.4426950408889634
VMEM = 67043328
SLOTS = 11
JOIN = 3
AHEAD = 6
PIECES = 8
MESH = pl.DeviceIdType.MESH

STEPS = [(1, 1), (3, 3), (1, 3), (3, 1), (1, 0), (3, 0), (0, 1), (0, 3), (1, 2), (3, 2), (2, 1), (2, 3), (2, 2), (2, 0), (0, 2), (0, 0)]
UNITS = [(3, 0), (1, 0), (0, 0), (3, 1), (1, 1), (2, 1), (2, 0), (0, 1)]
LAST_ROW, OTHER_ROWS = [3, 2, 0, 1], [1, 3, 0, 2]


def _packed(values):
    return sum(v << (2 * i) for i, v in enumerate(values))


def _look(word, i):
    return lax.shift_right_logical(jnp.asarray(word, jnp.int32), 2 * i) & 3


def _step(axis, t):
    low, high = (_packed([s[axis] for s in STEPS[at : at + 8]]) for at in (0, 8))
    return lax.shift_right_logical(jnp.where(t < 8, jnp.int32(low), jnp.int32(high)), 2 * lax.rem(t, 8)) & 3


def _dot(a, b):
    return jnp.dot(a, b, preferred_element_type=jnp.float32)


def _kernel(n, x_hbm, gain_ref, rate_ref, wq, wk, wv, wo, y_ref,
            x_ref, cos_ref, sin_ref, a_s, w_s, k_out, v_out, q_out, k_in, v_in, q_in, o_out, o_in, even_s, odd_s, mix_s, top_s, sum_s,
            x_sem, w_sem, y_sem, k_sent, k_got, v_sent, v_got, q_sent, q_got, o_sent, o_got):
    own, depth = x_ref.shape
    features = wo.shape[0]
    hk, hq = k_out.shape[2], o_out.shape[2]
    g = hq // hk
    cols = g * own
    bk = even_s.shape[0]
    per = bk // own
    blocks = depth // hq
    me = lax.axis_index("sp")
    e = hk**-0.5 * LOG2E

    side = math.isqrt(n)
    mx, my = lax.div(me, side), lax.rem(me, side)
    row = features // side

    def target(t):
        return lax.rem(mx + _step(0, t), side) * side + lax.rem(my + _step(1, t), side)

    def unit(i):
        flip = _look(_packed([s[1] for s in UNITS]), i)
        return lax.div(lax.rem(mx + _look(_packed([s[0] for s in UNITS]), i), side) * side, per) + (lax.div(my, per) ^ flip)

    def place(to, frm):
        return lax.rem(lax.div(frm, side) - lax.div(to, side) + side, side) * side + lax.rem(frm, side)

    def turn(c):
        return _look(jnp.where(mx == side - 1, jnp.int32(_packed(LAST_ROW)), jnp.int32(_packed(OTHER_ROWS))), c)

    halves = 2

    def x_copy(i):
        at = pl.ds(i * (own // halves), own // halves)
        return pltpu.make_async_copy(x_hbm.at[at, :], x_ref.at[at, :], x_sem.at[i])

    for i in range(halves):
        x_copy(i).start()
    barrier = pltpu.get_barrier_semaphore()
    for s in range(1, n):
        pl.semaphore_signal(barrier, inc=1, device_id={"sp": lax.rem(me + s, n)}, device_id_type=MESH)

    def fetch_kv(t):
        slot, at = lax.rem(t, SLOTS), pl.ds(pl.multiple_of(target(t) * hk, hk), hk)
        pltpu.make_async_copy(wk.at[:, at], w_s.at[slot, pl.ds(0, depth), pl.ds(0, hk)], w_sem.at[slot]).start()
        pltpu.make_async_copy(wv.at[:, at], w_s.at[slot, pl.ds(0, depth), pl.ds(hk, hk)], w_sem.at[slot]).start()

    def q_copy(t):
        slot, at = lax.rem(t, SLOTS), pl.ds(pl.multiple_of(target(t - n) * hq, hq), hq)
        return pltpu.make_async_copy(wq.at[:, at], w_s.at[slot, pl.ds(0, depth), :], w_sem.at[slot])

    joined = blocks // JOIN
    jobs = side * joined

    def o_slot(j):
        return lax.rem(j + 2 * n, SLOTS)

    def fetch_o(j):
        frm = pl.multiple_of(lax.rem(mx + turn(lax.div(j, joined)), side) * row, row)
        for b in range(JOIN):
            at = pl.ds(pl.multiple_of((lax.rem(j, joined) * JOIN + b) * hq, hq), hq)
            pltpu.make_async_copy(wo.at[pl.ds(frm, row), at], w_s.at[o_slot(j), pl.ds(b * row, row), :], w_sem.at[o_slot(j)]).start()

    def o_here(j):
        slot, rows = o_slot(j), pl.ds(0, JOIN * row)
        pltpu.make_async_copy(wo.at[rows, pl.ds(0, hq)], w_s.at[slot, rows, :], w_sem.at[slot]).wait()
        return slot

    lax.fori_loop(0, AHEAD, lambda t, _: fetch_kv(t), None)

    rows = 16

    def norm(r, _):
        at = pl.ds(pl.multiple_of(r * rows, rows), rows)
        wide = x_ref[at, :].astype(jnp.float32)
        scale = lax.rsqrt(jnp.mean(wide * wide, -1, keepdims=True) + 1e-6)
        a_s[at, :] = (wide * scale * gain_ref[...].astype(jnp.float32)[None]).astype(a_s.dtype)

    place_f = (me * own + lax.broadcasted_iota(jnp.int32, (own, hk), 0)).astype(jnp.float32)
    angle = place_f * rate_ref[...]
    cos_ref[...] = jnp.cos(angle)
    sine = jnp.sin(angle)
    sin_ref[...] = jnp.where(lax.broadcasted_iota(jnp.int32, (own, hk), 1) < hk // 2, -sine, sine)
    each = own // rows // halves
    for i in range(halves):
        x_copy(i).wait()
        lax.fori_loop(i * each, (i + 1) * each, norm, None, unroll=4)
    v_in[:, hk:, :] = jnp.ones((n, v_in.shape[1] - hk, own), v_in.dtype)
    pl.semaphore_wait(barrier, n - 1)

    def turned(t):
        wide = t.astype(jnp.float32)
        return (wide * cos_ref[...] + pltpu.roll(wide, hk // 2, 1) * sin_ref[...]).astype(t.dtype)

    def send(src, dst, sent, got, to, frm):
        return pltpu.make_async_remote_copy(src_ref=src, dst_ref=dst, send_sem=sent.at[to], recv_sem=got.at[frm],
                                            device_id={"sp": to}, device_id_type=MESH)

    def k_send(to, frm):
        return send(k_out.at[to], k_in.at[frm], k_sent, k_got, to, frm)

    def v_send(to, frm):
        return send(v_out.at[to], v_in.at[frm, pl.ds(0, hk), :], v_sent, v_got, to, frm)

    def q_send(to, frm):
        return send(q_out.at[to], q_in.at[frm], q_sent, q_got, to, frm)

    def o_send(to, frm):
        return send(o_out.at[to], o_in.at[place(to, frm)], o_sent, o_got, to, frm)

    def block_here(t):
        slot = lax.rem(t, SLOTS)
        pltpu.make_async_copy(wq.at[:, pl.ds(0, hq)], w_s.at[slot, pl.ds(0, depth), :], w_sem.at[slot]).wait()
        return slot

    def made(t):
        return _dot(a_s[...], w_s[lax.rem(t, SLOTS), :depth, :]).astype(a_s.dtype)

    def keys_values(i, _):
        for t in (2 * i, 2 * i + 1):
            @pl.when(t + AHEAD < n)
            def _():
                fetch_kv(t + AHEAD)

            @pl.when(t + AHEAD >= n)
            def _():
                q_copy(t + AHEAD).start()

        @pl.when(i > 0)
        def _():
            before = target(jnp.maximum(2 * i - 1, 0))
            k_send(before, me).start()
            v_send(before, me).start()

        for t in (2 * i, 2 * i + 1):
            block_here(t)

        def finish(to, r):
            k_out[to] = turned(r[:, :hk])
            v_out[to] = r[:, hk:].T

        first, second = target(2 * i), target(2 * i + 1)
        finish(first, made(2 * i))
        r = made(2 * i + 1)
        k_send(first, me).start()
        v_send(first, me).start()
        finish(second, r)

    lax.fori_loop(0, n // 2, keys_values, None)
    k_in[me] = k_out[me]
    v_in[me, :hk, :] = v_out[me]

    def queries(i, _):
        for t in (2 * i, 2 * i + 1):
            @pl.when(t + n + AHEAD < 2 * n)
            def _():
                q_copy(t + n + AHEAD).start()

            @pl.when(t + n + AHEAD >= 2 * n)
            def _():
                fetch_o(t + AHEAD - n)

        @pl.when(i > 0)
        def _():
            q_send(target(jnp.maximum(2 * i - 1, 0)), me).start()

        for t in (2 * i, 2 * i + 1):
            block_here(t + n)

        def finish(to, r):
            for h in range(g):
                q_out[to, :, h * own : (h + 1) * own] = turned(r[:, h * hk : (h + 1) * hk]).T

        first, second = target(2 * i), target(2 * i + 1)
        finish(first, made(2 * i + n))
        r = made(2 * i + 1 + n)
        q_send(first, me).start()
        finish(second, r)

    lax.fori_loop(0, n // 2, queries, None)
    q_in[me] = q_out[me]

    def got_keys(s, _):
        frm = target(s)
        k_send(frm, frm).wait_recv()
        v_send(frm, frm).wait_recv()

    lax.fori_loop(0, n - 1, got_keys, None)

    def attend(s, _):
        u = unit(s)

        @pl.when(AHEAD + s < SLOTS)
        def _():
            fetch_o(AHEAD + s)

        @pl.when(s > 0)
        def _():
            send_out(jnp.maximum(s - 1, 0))

        for c in range(per):
            @pl.when(per * u + c != me)
            def _():
                q_send(per * u + c, per * u + c).wait_recv()

        def scores(j, into):
            keys = jnp.concatenate([k_in[j * per + c] for c in range(per)], axis=0)
            for c in range(per):
                into[:, c * cols : (c + 1) * cols] = _dot(keys, q_in[u * per + c])

        def take(j, held, masked):
            weights, keeps = [], []
            for c in range(per):
                at = slice(c * cols, (c + 1) * cols)
                sc = held[:, at]
                if masked:
                    query = lax.rem(lax.broadcasted_iota(jnp.int32, (bk, cols), 1), own) + c * own
                    sc = jnp.where(query >= lax.broadcasted_iota(jnp.int32, (bk, cols), 0), sc, HIDDEN)
                old = top_s[:, at]
                new = jnp.maximum(old, sc.max(axis=0, keepdims=True))
                top_s[:, at] = new
                weights.append(jnp.exp2((sc - new) * e).astype(k_in.dtype))
                keeps.append(jnp.exp2((old - new) * e))
            values = jnp.concatenate([v_in[j * per + c] for c in range(per)], axis=1)
            for c in range(per):
                at = slice(c * cols, (c + 1) * cols)
                mix_s[:, at] = mix_s[:, at] * keeps[c] + _dot(values, weights[c])

        scores(0, even_s)

        mix_s[...] = jnp.zeros_like(mix_s)
        top_s[...] = jnp.full_like(top_s, NEG)

        def two(i, _):
            scores(2 * i + 1, odd_s)
            take(2 * i, even_s, False)
            scores(2 * i + 2, even_s)
            take(2 * i + 1, odd_s, False)

        lax.fori_loop(0, lax.div(u, 2), two, None)

        @pl.when(lax.rem(u, 2) == 1)
        def _():
            scores(u, odd_s)
            take(u - 1, even_s, False)
            take(u, odd_s, True)

        @pl.when(lax.rem(u, 2) == 0)
        def _():
            take(u, even_s, True)

        for c in range(per):
            at = slice(c * cols, (c + 1) * cols)
            out = (mix_s[:hk, at] * (1 / mix_s[hk : hk + 1, at])).astype(o_in.dtype)
            o_out[per * u + c] = jnp.concatenate([out[:, h * own : (h + 1) * own].T for h in range(g)], axis=1)

    def send_out(s):
        u = unit(s)
        for c in range(per):
            @pl.when(per * u + c != me)
            def _():
                o_send(per * u + c, me).start()

    lax.fori_loop(0, n // 2, attend, None)
    send_out(n // 2 - 1)
    o_in[place(me, me)] = o_out[me]

    def got_out(c):
        def got(y, _):
            frm = lax.rem(mx + turn(c), side) * side + y

            @pl.when(frm != me)
            def _():
                pltpu.make_async_remote_copy(src_ref=o_out.at[frm], dst_ref=o_in.at[place(me, frm)], send_sem=o_sent.at[frm],
                                             recv_sem=o_got.at[frm], device_id={"sp": frm}, device_id_type=MESH).wait_recv()

        lax.fori_loop(0, side, got, None)

    def products(j, count):
        slots, first = [o_here(j + i) for i in range(count)], turn(lax.div(j, joined)) * side
        results = jnp.concatenate([o_in[first + y] for y in range(side)], axis=1)
        for i, slot in enumerate(slots):
            for b in range(JOIN):
                at = pl.ds(pl.multiple_of((lax.rem(j + i, joined) * JOIN + b) * hq, hq), hq)
                yield at, _dot(results, w_s[slot, b * row : (b + 1) * row, :])

    def by_twos(c, body):
        lax.fori_loop(0, joined // 2, lambda i, _: body(c * joined + 2 * i, 2), None)
        if joined % 2:
            body(c * joined + joined - 1, 1)

    def first_row(j, count):
        for at, r in products(j, count):
            sum_s[:, at] = x_ref[:, at].astype(jnp.float32) + r
        for i in range(count):
            fetch_o(j + i + SLOTS)

    def middle_row(j, count):
        for at, r in products(j, count):
            sum_s[:, at] += r
        for i in range(count):
            @pl.when(j + i + SLOTS < jobs)
            def _():
                fetch_o(j + i + SLOTS)

    got_out(0)
    by_twos(0, first_row)

    def between(c, _):
        got_out(c)
        by_twos(c, middle_row)

    lax.fori_loop(1, side - 1, between, None)
    got_out(side - 1)

    def y_copy(i):
        at = pl.ds(pl.multiple_of(i * JOIN * hq, JOIN * hq), JOIN * hq)
        return pltpu.make_async_copy(a_s.at[:, at], y_ref.at[:, at], y_sem.at[i])

    def last_row(j, count):
        at = j - (side - 1) * joined

        @pl.when(at > 0)
        def _():
            for i in (2, 1):
                y_copy(jnp.maximum(at - i, 0)).start()

        for columns, r in products(j, count):
            a_s[:, columns] = (sum_s[:, columns] + r).astype(a_s.dtype)

    by_twos(side - 1, last_row)
    for i in range(joined - 2 + joined % 2, joined):
        y_copy(i).start()

    def gone(s, _):
        to = target(s)
        k_send(to, me).wait_send()
        v_send(to, me).wait_send()
        q_send(to, me).wait_send()
        o_send(to, me).wait_send()

    lax.fori_loop(0, n - 1, gone, None)
    lax.fori_loop(0, joined, lambda i, _: y_copy(i).wait(), None)


def _copy(y_ref, out_ref, held, read, written):
    rows = held.shape[0] // PIECES

    def into(i):
        at = pl.ds(i * rows, rows)
        return pltpu.make_async_copy(y_ref.at[at, :], held.at[at, :], read.at[i])

    def out(i):
        at = pl.ds(i * rows, rows)
        return pltpu.make_async_copy(held.at[at, :], out_ref.at[at, :], written.at[i])

    for i in range(PIECES):
        into(i).start()
    for i in range(PIECES):
        into(i).wait()
        out(i).start()
    for i in range(PIECES):
        out(i).wait()


def solution(mesh):
    n = mesh.shape["sp"]

    def step(x, gain, wq, wk, wv, wo):
        own, depth = x.shape
        hq, hk, features = wq.shape[1] // n, wk.shape[1] // n, wo.shape[0]
        g = hq // hk
        low = x.dtype
        half = HEAD // 2
        rate = THETA ** (-jnp.arange(half, dtype=jnp.float32) / half)
        rate = jnp.concatenate([rate, rate])[None]
        bk = 2 * own
        sems = pltpu.SemaphoreType.DMA((n,))
        vmem, hbm = pl.BlockSpec(memory_space=pltpu.VMEM), pl.BlockSpec(memory_space=pl.ANY)
        y = pl.pallas_call(
            functools.partial(_kernel, n),
            name="half_layer",
            out_shape=jax.ShapeDtypeStruct((own, depth), low),
            in_specs=[hbm] + [vmem] * 2 + [hbm] * 4,
            out_specs=hbm,
            scratch_shapes=[
                pltpu.VMEM((own, depth), low),
                pltpu.VMEM((own, hk), jnp.float32),
                pltpu.VMEM((own, hk), jnp.float32),
                pltpu.VMEM((own, depth), low),
                pltpu.VMEM((SLOTS, max(depth, features), hq), low),
                pltpu.VMEM((n, own, hk), low),
                pltpu.VMEM((n, hk, own), low),
                pltpu.VMEM((n, hk, g * own), low),
                pltpu.VMEM((n, own, hk), low),
                pltpu.VMEM((n, hk + 16, own), low),
                pltpu.VMEM((n, hk, g * own), low),
                pltpu.VMEM((n, own, hq), low),
                pltpu.VMEM((n, own, hq), low),
                pltpu.VMEM((bk, 2 * g * own), jnp.float32),
                pltpu.VMEM((bk, 2 * g * own), jnp.float32),
                pltpu.VMEM((hk + 16, 2 * g * own), jnp.float32),
                pltpu.VMEM((1, 2 * g * own), jnp.float32),
                pltpu.VMEM((own, depth), jnp.float32),
                pltpu.SemaphoreType.DMA((2,)),
                pltpu.SemaphoreType.DMA((SLOTS,)),
                pltpu.SemaphoreType.DMA((depth // hq // JOIN,)),
            ] + [sems] * 8,
            compiler_params=pltpu.CompilerParams(collective_id=0, has_side_effects=True, vmem_limit_bytes=VMEM),
        )(x, gain, rate, wq, wk, wv, wo)
        return pl.pallas_call(
            _copy,
            name="result",
            out_shape=jax.ShapeDtypeStruct((own, depth), low),
            in_specs=[hbm],
            out_specs=hbm,
            scratch_shapes=[pltpu.VMEM((own, depth), low), pltpu.SemaphoreType.DMA((PIECES,)), pltpu.SemaphoreType.DMA((PIECES,))],
            compiler_params=pltpu.CompilerParams(vmem_limit_bytes=VMEM),
        )(y)

    tokens, whole = P(("dp", "sp"), None), P(None, None)
    return jax.shard_map(
        step,
        mesh=mesh,
        in_specs=(tokens, P(None), whole, whole, whole, whole),
        out_specs=tokens,
        check_vma=False,
    )
```

```python
import functools
import math

import jax
import jax.numpy as jnp
from jax import lax
from jax.experimental import pallas as pl
from jax.experimental.pallas import tpu as pltpu
from jax.sharding import PartitionSpec as P

HEAD = 128
THETA = 10000
NEG = -1e30
HIDDEN = 2 * NEG
LOG2E = 1.4426950408889634
VMEM = 67043328
SLOTS = 11
JOIN = 3
AHEAD = 6
PIECES = 8
MESH = pl.DeviceIdType.MESH

STEPS = [(1, 1), (3, 3), (1, 3), (3, 1), (1, 0), (3, 0), (0, 1), (0, 3), (1, 2), (3, 2), (2, 1), (2, 3), (2, 2), (2, 0), (0, 2), (0, 0)]
UNITS = [(3, 0), (1, 0), (0, 0), (3, 1), (1, 1), (2, 1), (2, 0), (0, 1)]
LAST_ROW, OTHER_ROWS = [3, 2, 0, 1], [1, 3, 0, 2]


def _packed(values):
    return sum(v << (2 * i) for i, v in enumerate(values))


def _look(word, i):
    return lax.shift_right_logical(jnp.asarray(word, jnp.int32), 2 * i) & 3


def _step(axis, t):
    low, high = (_packed([s[axis] for s in STEPS[at : at + 8]]) for at in (0, 8))
    return lax.shift_right_logical(jnp.where(t < 8, jnp.int32(low), jnp.int32(high)), 2 * lax.rem(t, 8)) & 3


def _dot(a, b):
    return jnp.dot(a, b, preferred_element_type=jnp.float32)


def _kernel(n, x_ref, gain_ref, cos_ref, sin_ref, wq, wk, wv, wo, y_ref,
            a_s, w_s, k_out, v_out, q_out, k_in, v_in, q_in, o_out, o_in, even_s, odd_s, mix_s, top_s, sum_s,
            w_sem, y_sem, k_sent, k_got, v_sent, v_got, q_sent, q_got, o_sent, o_got):
    own, depth = x_ref.shape
    features = wo.shape[0]
    hk, hq = k_out.shape[2], o_out.shape[2]
    g = hq // hk
    cols = g * own
    bk = even_s.shape[0]
    per = bk // own
    blocks = depth // hq
    me = lax.axis_index("sp")
    e = hk**-0.5 * LOG2E

    side = math.isqrt(n)
    mx, my = lax.div(me, side), lax.rem(me, side)
    row = features // side

    def target(t):
        return lax.rem(mx + _step(0, t), side) * side + lax.rem(my + _step(1, t), side)

    def unit(i):
        flip = _look(_packed([s[1] for s in UNITS]), i)
        return lax.div(lax.rem(mx + _look(_packed([s[0] for s in UNITS]), i), side) * side, per) + (lax.div(my, per) ^ flip)

    def place(to, frm):
        return lax.rem(lax.div(frm, side) - lax.div(to, side) + side, side) * side + lax.rem(frm, side)

    def turn(c):
        return _look(jnp.where(mx == side - 1, jnp.int32(_packed(LAST_ROW)), jnp.int32(_packed(OTHER_ROWS))), c)

    barrier = pltpu.get_barrier_semaphore()
    for s in range(1, n):
        pl.semaphore_signal(barrier, inc=1, device_id={"sp": lax.rem(me + s, n)}, device_id_type=MESH)

    def fetch_kv(t):
        slot, at = lax.rem(t, SLOTS), pl.ds(pl.multiple_of(target(t) * hk, hk), hk)
        pltpu.make_async_copy(wk.at[:, at], w_s.at[slot, pl.ds(0, depth), pl.ds(0, hk)], w_sem.at[slot]).start()
        pltpu.make_async_copy(wv.at[:, at], w_s.at[slot, pl.ds(0, depth), pl.ds(hk, hk)], w_sem.at[slot]).start()

    def q_copy(t):
        slot, at = lax.rem(t, SLOTS), pl.ds(pl.multiple_of(target(t - n) * hq, hq), hq)
        return pltpu.make_async_copy(wq.at[:, at], w_s.at[slot, pl.ds(0, depth), :], w_sem.at[slot])

    joined = blocks // JOIN
    jobs = side * joined

    def o_slot(j):
        return lax.rem(j + 2 * n, SLOTS)

    def fetch_o(j):
        frm = pl.multiple_of(lax.rem(mx + turn(lax.div(j, joined)), side) * row, row)
        for b in range(JOIN):
            at = pl.ds(pl.multiple_of((lax.rem(j, joined) * JOIN + b) * hq, hq), hq)
            pltpu.make_async_copy(wo.at[pl.ds(frm, row), at], w_s.at[o_slot(j), pl.ds(b * row, row), :], w_sem.at[o_slot(j)]).start()

    def o_here(j):
        slot, rows = o_slot(j), pl.ds(0, JOIN * row)
        pltpu.make_async_copy(wo.at[rows, pl.ds(0, hq)], w_s.at[slot, rows, :], w_sem.at[slot]).wait()
        return slot

    lax.fori_loop(0, AHEAD, lambda t, _: fetch_kv(t), None)

    rows = 16

    def norm(r, _):
        at = pl.ds(pl.multiple_of(r * rows, rows), rows)
        wide = x_ref[at, :].astype(jnp.float32)
        scale = lax.rsqrt(jnp.mean(wide * wide, -1, keepdims=True) + 1e-6)
        a_s[at, :] = (wide * scale * gain_ref[...].astype(jnp.float32)[None]).astype(a_s.dtype)

    lax.fori_loop(0, own // rows, norm, None, unroll=4)
    v_in[:, hk:, :] = jnp.ones((n, v_in.shape[1] - hk, own), v_in.dtype)
    pl.semaphore_wait(barrier, n - 1)

    def turned(t):
        wide = t.astype(jnp.float32)
        return (wide * cos_ref[...] + pltpu.roll(wide, hk // 2, 1) * sin_ref[...]).astype(t.dtype)

    def send(src, dst, sent, got, to, frm):
        return pltpu.make_async_remote_copy(src_ref=src, dst_ref=dst, send_sem=sent.at[to], recv_sem=got.at[frm],
                                            device_id={"sp": to}, device_id_type=MESH)

    def k_send(to, frm):
        return send(k_out.at[to], k_in.at[frm], k_sent, k_got, to, frm)

    def v_send(to, frm):
        return send(v_out.at[to], v_in.at[frm, pl.ds(0, hk), :], v_sent, v_got, to, frm)

    def q_send(to, frm):
        return send(q_out.at[to], q_in.at[frm], q_sent, q_got, to, frm)

    def o_send(to, frm):
        return send(o_out.at[to], o_in.at[place(to, frm)], o_sent, o_got, to, frm)

    def block_here(t):
        slot = lax.rem(t, SLOTS)
        pltpu.make_async_copy(wq.at[:, pl.ds(0, hq)], w_s.at[slot, pl.ds(0, depth), :], w_sem.at[slot]).wait()
        return slot

    def made(t):
        return _dot(a_s[...], w_s[lax.rem(t, SLOTS), :depth, :]).astype(a_s.dtype)

    def keys_values(i, _):
        for t in (2 * i, 2 * i + 1):
            @pl.when(t + AHEAD < n)
            def _():
                fetch_kv(t + AHEAD)

            @pl.when(t + AHEAD >= n)
            def _():
                q_copy(t + AHEAD).start()

        @pl.when(i > 0)
        def _():
            before = target(jnp.maximum(2 * i - 1, 0))
            k_send(before, me).start()
            v_send(before, me).start()

        for t in (2 * i, 2 * i + 1):
            block_here(t)

        def finish(to, r):
            k_out[to] = turned(r[:, :hk])
            v_out[to] = r[:, hk:].T

        first, second = target(2 * i), target(2 * i + 1)
        finish(first, made(2 * i))
        r = made(2 * i + 1)
        k_send(first, me).start()
        v_send(first, me).start()
        finish(second, r)

    lax.fori_loop(0, n // 2, keys_values, None)
    k_in[me] = k_out[me]
    v_in[me, :hk, :] = v_out[me]

    def queries(i, _):
        for t in (2 * i, 2 * i + 1):
            @pl.when(t + n + AHEAD < 2 * n)
            def _():
                q_copy(t + n + AHEAD).start()

            @pl.when(t + n + AHEAD >= 2 * n)
            def _():
                fetch_o(t + AHEAD - n)

        @pl.when(i > 0)
        def _():
            q_send(target(jnp.maximum(2 * i - 1, 0)), me).start()

        for t in (2 * i, 2 * i + 1):
            block_here(t + n)

        def finish(to, r):
            for h in range(g):
                q_out[to, :, h * own : (h + 1) * own] = turned(r[:, h * hk : (h + 1) * hk]).T

        first, second = target(2 * i), target(2 * i + 1)
        finish(first, made(2 * i + n))
        r = made(2 * i + 1 + n)
        q_send(first, me).start()
        finish(second, r)

    lax.fori_loop(0, n // 2, queries, None)
    q_in[me] = q_out[me]

    def got_keys(s, _):
        frm = target(s)
        k_send(frm, frm).wait_recv()
        v_send(frm, frm).wait_recv()

    lax.fori_loop(0, n - 1, got_keys, None)

    def attend(s, _):
        u = unit(s)

        @pl.when(AHEAD + s < SLOTS)
        def _():
            fetch_o(AHEAD + s)

        @pl.when(s > 0)
        def _():
            send_out(jnp.maximum(s - 1, 0))

        for c in range(per):
            @pl.when(per * u + c != me)
            def _():
                q_send(per * u + c, per * u + c).wait_recv()

        def scores(j, into):
            keys = jnp.concatenate([k_in[j * per + c] for c in range(per)], axis=0)
            for c in range(per):
                into[:, c * cols : (c + 1) * cols] = _dot(keys, q_in[u * per + c])

        def take(j, held, masked):
            weights, keeps = [], []
            for c in range(per):
                at = slice(c * cols, (c + 1) * cols)
                sc = held[:, at]
                if masked:
                    query = lax.rem(lax.broadcasted_iota(jnp.int32, (bk, cols), 1), own) + c * own
                    sc = jnp.where(query >= lax.broadcasted_iota(jnp.int32, (bk, cols), 0), sc, HIDDEN)
                old = top_s[:, at]
                new = jnp.maximum(old, sc.max(axis=0, keepdims=True))
                top_s[:, at] = new
                weights.append(jnp.exp2((sc - new) * e).astype(k_in.dtype))
                keeps.append(jnp.exp2((old - new) * e))
            values = jnp.concatenate([v_in[j * per + c] for c in range(per)], axis=1)
            for c in range(per):
                at = slice(c * cols, (c + 1) * cols)
                mix_s[:, at] = mix_s[:, at] * keeps[c] + _dot(values, weights[c])

        scores(0, even_s)

        mix_s[...] = jnp.zeros_like(mix_s)
        top_s[...] = jnp.full_like(top_s, NEG)

        def two(i, _):
            scores(2 * i + 1, odd_s)
            take(2 * i, even_s, False)
            scores(2 * i + 2, even_s)
            take(2 * i + 1, odd_s, False)

        lax.fori_loop(0, lax.div(u, 2), two, None)

        @pl.when(lax.rem(u, 2) == 1)
        def _():
            scores(u, odd_s)
            take(u - 1, even_s, False)
            take(u, odd_s, True)

        @pl.when(lax.rem(u, 2) == 0)
        def _():
            take(u, even_s, True)

        for c in range(per):
            at = slice(c * cols, (c + 1) * cols)
            out = (mix_s[:hk, at] * (1 / mix_s[hk : hk + 1, at])).astype(o_in.dtype)
            o_out[per * u + c] = jnp.concatenate([out[:, h * own : (h + 1) * own].T for h in range(g)], axis=1)

    def send_out(s):
        u = unit(s)
        for c in range(per):
            @pl.when(per * u + c != me)
            def _():
                o_send(per * u + c, me).start()

    lax.fori_loop(0, n // 2, attend, None)
    send_out(n // 2 - 1)
    o_in[place(me, me)] = o_out[me]

    def got_out(c):
        def got(y, _):
            frm = lax.rem(mx + turn(c), side) * side + y

            @pl.when(frm != me)
            def _():
                pltpu.make_async_remote_copy(src_ref=o_out.at[frm], dst_ref=o_in.at[place(me, frm)], send_sem=o_sent.at[frm],
                                             recv_sem=o_got.at[frm], device_id={"sp": frm}, device_id_type=MESH).wait_recv()

        lax.fori_loop(0, side, got, None)

    def products(j, count):
        slots, first = [o_here(j + i) for i in range(count)], turn(lax.div(j, joined)) * side
        results = jnp.concatenate([o_in[first + y] for y in range(side)], axis=1)
        for i, slot in enumerate(slots):
            for b in range(JOIN):
                at = pl.ds(pl.multiple_of((lax.rem(j + i, joined) * JOIN + b) * hq, hq), hq)
                yield at, _dot(results, w_s[slot, b * row : (b + 1) * row, :])

    def by_twos(c, body):
        lax.fori_loop(0, joined // 2, lambda i, _: body(c * joined + 2 * i, 2), None)
        if joined % 2:
            body(c * joined + joined - 1, 1)

    def first_row(j, count):
        for at, r in products(j, count):
            sum_s[:, at] = x_ref[:, at].astype(jnp.float32) + r
        for i in range(count):
            fetch_o(j + i + SLOTS)

    def middle_row(j, count):
        for at, r in products(j, count):
            sum_s[:, at] += r
        for i in range(count):
            @pl.when(j + i + SLOTS < jobs)
            def _():
                fetch_o(j + i + SLOTS)

    got_out(0)
    by_twos(0, first_row)

    def between(c, _):
        got_out(c)
        by_twos(c, middle_row)

    lax.fori_loop(1, side - 1, between, None)
    got_out(side - 1)

    def y_copy(i):
        at = pl.ds(pl.multiple_of(i * JOIN * hq, JOIN * hq), JOIN * hq)
        return pltpu.make_async_copy(a_s.at[:, at], y_ref.at[:, at], y_sem.at[i])

    def last_row(j, count):
        at = j - (side - 1) * joined

        @pl.when(at > 0)
        def _():
            for i in (2, 1):
                y_copy(jnp.maximum(at - i, 0)).start()

        for columns, r in products(j, count):
            a_s[:, columns] = (sum_s[:, columns] + r).astype(a_s.dtype)

    by_twos(side - 1, last_row)
    for i in range(joined - 2 + joined % 2, joined):
        y_copy(i).start()

    def gone(s, _):
        to = target(s)
        k_send(to, me).wait_send()
        v_send(to, me).wait_send()
        q_send(to, me).wait_send()
        o_send(to, me).wait_send()

    lax.fori_loop(0, n - 1, gone, None)
    lax.fori_loop(0, joined, lambda i, _: y_copy(i).wait(), None)


def _copy(y_ref, out_ref, held, read, written):
    rows = held.shape[0] // PIECES

    def into(i):
        at = pl.ds(i * rows, rows)
        return pltpu.make_async_copy(y_ref.at[at, :], held.at[at, :], read.at[i])

    def out(i):
        at = pl.ds(i * rows, rows)
        return pltpu.make_async_copy(held.at[at, :], out_ref.at[at, :], written.at[i])

    for i in range(PIECES):
        into(i).start()
    for i in range(PIECES):
        into(i).wait()
        out(i).start()
    for i in range(PIECES):
        out(i).wait()


def solution(mesh):
    n = mesh.shape["sp"]

    def step(x, gain, wq, wk, wv, wo):
        own, depth = x.shape
        hq, hk, features = wq.shape[1] // n, wk.shape[1] // n, wo.shape[0]
        g = hq // hk
        low = x.dtype
        half = HEAD // 2
        place = (lax.axis_index("sp") * own + jnp.arange(own)).astype(jnp.float32)
        angle = place[:, None] * THETA ** (-jnp.arange(half, dtype=jnp.float32) / half)
        cos, sin = jnp.cos(angle), jnp.sin(angle)
        cos, sin = jnp.concatenate([cos, cos], -1), jnp.concatenate([-sin, sin], -1)
        bk = 2 * own
        sems = pltpu.SemaphoreType.DMA((n,))
        vmem, hbm = pl.BlockSpec(memory_space=pltpu.VMEM), pl.BlockSpec(memory_space=pl.ANY)
        y = pl.pallas_call(
            functools.partial(_kernel, n),
            name="half_layer",
            out_shape=jax.ShapeDtypeStruct((own, depth), low),
            in_specs=[vmem] * 4 + [hbm] * 4,
            out_specs=hbm,
            scratch_shapes=[
                pltpu.VMEM((own, depth), low),
                pltpu.VMEM((SLOTS, max(depth, features), hq), low),
                pltpu.VMEM((n, own, hk), low),
                pltpu.VMEM((n, hk, own), low),
                pltpu.VMEM((n, hk, g * own), low),
                pltpu.VMEM((n, own, hk), low),
                pltpu.VMEM((n, hk + 16, own), low),
                pltpu.VMEM((n, hk, g * own), low),
                pltpu.VMEM((n, own, hq), low),
                pltpu.VMEM((n, own, hq), low),
                pltpu.VMEM((bk, 2 * g * own), jnp.float32),
                pltpu.VMEM((bk, 2 * g * own), jnp.float32),
                pltpu.VMEM((hk + 16, 2 * g * own), jnp.float32),
                pltpu.VMEM((1, 2 * g * own), jnp.float32),
                pltpu.VMEM((own, depth), jnp.float32),
                pltpu.SemaphoreType.DMA((SLOTS,)),
                pltpu.SemaphoreType.DMA((depth // hq // JOIN,)),
            ] + [sems] * 8,
            compiler_params=pltpu.CompilerParams(collective_id=0, has_side_effects=True, vmem_limit_bytes=VMEM),
        )(x, gain, cos, sin, wq, wk, wv, wo)
        return pl.pallas_call(
            _copy,
            name="result",
            out_shape=jax.ShapeDtypeStruct((own, depth), low),
            in_specs=[hbm],
            out_specs=hbm,
            scratch_shapes=[pltpu.VMEM((own, depth), low), pltpu.SemaphoreType.DMA((PIECES,)), pltpu.SemaphoreType.DMA((PIECES,))],
            compiler_params=pltpu.CompilerParams(vmem_limit_bytes=VMEM),
        )(y)

    tokens, whole = P(("dp", "sp"), None), P(None, None)
    return jax.shard_map(
        step,
        mesh=mesh,
        in_specs=(tokens, P(None), whole, whole, whole, whole),
        out_specs=tokens,
        check_vma=False,
    )
```
